8 devices in a mesh: pod: 1 (over z), dp: 2 (over y), stage: 4 (over x, core).
Axes of the slice: x: 2, y: 2, z: 1, core: 2. Of those that a mesh axis runs over, the one named last changes fastest.
Arguments:
- x_emb: bfloat16 [4, 512, 2048], P(None, ('pod', 'dp'))
- labels: int32 [4, 512], P(None, ('pod', 'dp'))
- norm_gain: float32 [4, 1, 2048], P(('pod', 'stage'))
- w_up: bfloat16 [4, 1, 2048, 8192], P(('pod', 'stage'))
- w_down: bfloat16 [4, 1, 8192, 2048], P(('pod', 'stage'))
- w_out: bfloat16 [49152, 2048], P(('pod', 'stage'))
Outputs:
- output 1: float32 [1], P('pod')
- output 2: float32 [4, 512, 2048], P(None, ('pod', 'dp'), 'stage')
- output 3: float32 [4, 1, 2048], P(('pod', 'stage'))
- output 4: float32 [4, 1, 2048, 8192], P(('pod', 'stage'))
- output 5: float32 [4, 1, 8192, 2048], P(('pod', 'stage'))
- output 6: float32 [49152, 2048], P(('pod', 'stage'))
All inputs are finite; a program needn't handle non-finite values.
Results may differ from the reference program's by a relative error of at most 0.02.
Values are sent between devices in bfloat16 or wider.
A program may use at most 1.5 GiB of HBM per device.

```python
import jax
import jax.numpy as jnp
from jax import lax

MICRO_BATCHES = 4
TOK_DEV = 256
DP_SIZE = 2
STAGES = 4
LAYERS = 1
D_MODEL = 2048
FF_DIM = 8192
VOCAB = 49152

TOKENS = DP_SIZE * TOK_DEV
NORM_EPS = 1e-6


def setup_inputs(seed: int = 0, part: int = 0) -> dict:
    base_key = jax.random.fold_in(jax.random.key(seed), part)
    sub_keys = jax.random.split(base_key, 6)
    n_depth = STAGES * LAYERS
    x_emb = jax.random.normal(sub_keys[0], (MICRO_BATCHES, TOKENS, D_MODEL), jnp.float32)
    labels = jax.random.randint(sub_keys[1], (MICRO_BATCHES, TOKENS), 0, VOCAB, jnp.int32)
    norm_gain = 1.0 + 0.3 * jax.random.normal(sub_keys[2], (STAGES, LAYERS, D_MODEL), jnp.float32)
    w_up = jax.random.normal(sub_keys[3], (STAGES, LAYERS, D_MODEL, FF_DIM), jnp.float32) * D_MODEL ** -0.5
    w_down = jax.random.normal(sub_keys[4], (STAGES, LAYERS, FF_DIM, D_MODEL), jnp.float32) * (2.0 * (FF_DIM * n_depth) ** -0.5)
    w_out = jax.random.normal(sub_keys[5], (VOCAB, D_MODEL), jnp.float32) * (2.0 * D_MODEL ** -0.5)
    return {'x_emb': x_emb.astype(jnp.bfloat16), 'labels': labels, 'norm_gain': norm_gain, 'w_up': w_up.astype(jnp.bfloat16), 'w_down': w_down.astype(jnp.bfloat16), 'w_out': w_out.astype(jnp.bfloat16)}


def norm_apply(h_f32, gain_vec):
    inv_rms = lax.rsqrt(jnp.mean(h_f32 * h_f32, axis=-1, keepdims=True) + NORM_EPS)
    return h_f32 * inv_rms * gain_vec


def block_forward(h_in, gain_vec, w_up, w_down):
    h_f32 = h_in.astype(jnp.float32)
    normed = norm_apply(h_f32, gain_vec).astype(jnp.bfloat16)
    pre_act = jnp.dot(normed, w_up, preferred_element_type=jnp.float32)
    act_bf16 = jax.nn.gelu(pre_act).astype(jnp.bfloat16)
    return (h_f32 + jnp.dot(act_bf16, w_down, preferred_element_type=jnp.float32)).astype(jnp.bfloat16)


def block_backward(h_in, grad_out, gain_vec, w_up, w_down):
    h_f32 = h_in.astype(jnp.float32)
    normed_f, norm_vjp = jax.vjp(norm_apply, h_f32, gain_vec)
    normed = normed_f.astype(jnp.bfloat16)
    pre_act = jnp.dot(normed, w_up, preferred_element_type=jnp.float32)
    act_f, gelu_vjp = jax.vjp(jax.nn.gelu, pre_act)
    act_bf16 = act_f.astype(jnp.bfloat16)
    d_down = jnp.dot(act_bf16.T, grad_out, preferred_element_type=jnp.float32)
    d_act = jnp.dot(grad_out, w_down.T, preferred_element_type=jnp.float32)
    d_pre = gelu_vjp(d_act)[0].astype(jnp.bfloat16)
    d_up = jnp.dot(normed.T, d_pre, preferred_element_type=jnp.float32)
    d_normed = jnp.dot(d_pre, w_up.T, preferred_element_type=jnp.float32)
    d_h, d_gain = norm_vjp(d_normed)
    return grad_out.astype(jnp.float32) + d_h, d_gain, d_up, d_down


def reference(x_emb, labels, norm_gain, w_up, w_down, w_out):
    n_depth = STAGES * LAYERS
    gain_seq = norm_gain.reshape(n_depth, D_MODEL)
    up_seq = w_up.reshape(n_depth, D_MODEL, FF_DIM)
    down_seq = w_down.reshape(n_depth, FF_DIM, D_MODEL)
    x_blocks = x_emb.reshape(MICRO_BATCHES * DP_SIZE, TOK_DEV, D_MODEL)
    label_blocks = labels.reshape(MICRO_BATCHES * DP_SIZE, TOK_DEV)
    loss_scale = 1.0 / (MICRO_BATCHES * TOKENS)
    col_ids = jnp.arange(VOCAB, dtype=jnp.int32)

    def layer_fwd(h_in, layer_w):
        gain_vec, up_w, down_w = layer_w
        return block_forward(h_in, gain_vec, up_w, down_w), h_in

    def layer_bwd(grad_f, layer_w):
        h_in, gain_vec, up_w, down_w = layer_w
        grad_f, d_gain, d_up, d_down = block_backward(h_in, grad_f.astype(jnp.bfloat16), gain_vec, up_w, down_w)
        return grad_f, (d_gain, d_up, d_down)

    def token_block(state_in, block_in):
        loss_sum, acc_gain, acc_up, acc_down, acc_out = state_in
        x_blk, lab_blk = block_in
        h_final, layer_inputs = lax.scan(layer_fwd, x_blk, (gain_seq, up_seq, down_seq))
        logits = jnp.dot(h_final, w_out.T, preferred_element_type=jnp.float32)
        row_max = jnp.max(logits, axis=-1)
        log_norm = row_max + jnp.log(jnp.sum(jnp.exp(logits - row_max[:, None]), axis=-1))
        is_label = col_ids[None, :] == lab_blk[:, None]
        target = jnp.sum(jnp.where(is_label, logits, 0.0), axis=-1)
        softmax_p = jnp.exp(logits - log_norm[:, None])
        d_logits = ((softmax_p - is_label.astype(jnp.float32)) * loss_scale).astype(jnp.bfloat16)
        acc_out = acc_out + jnp.dot(d_logits.T, h_final, preferred_element_type=jnp.float32)
        d_final = jnp.dot(d_logits, w_out, preferred_element_type=jnp.float32)
        grad_x, layer_grads = lax.scan(layer_bwd, d_final, (layer_inputs, gain_seq, up_seq, down_seq), reverse=True)
        d_gain, d_up, d_down = layer_grads
        new_state = (loss_sum + jnp.sum(log_norm - target), acc_gain + d_gain, acc_up + d_up, acc_down + d_down, acc_out)
        return new_state, grad_x

    init_state = (jnp.zeros((), jnp.float32), jnp.zeros((n_depth, D_MODEL), jnp.float32), jnp.zeros((n_depth, D_MODEL, FF_DIM), jnp.float32), jnp.zeros((n_depth, FF_DIM, D_MODEL), jnp.float32), jnp.zeros((VOCAB, D_MODEL), jnp.float32))
    final_state, grad_x = lax.scan(token_block, init_state, (x_blocks, label_blocks))
    loss_sum, acc_gain, acc_up, acc_down, acc_out = final_state
    return ((loss_sum * loss_scale).reshape(1), grad_x.reshape(MICRO_BATCHES, TOKENS, D_MODEL), acc_gain.reshape(STAGES, LAYERS, D_MODEL), acc_up.reshape(STAGES, LAYERS, D_MODEL, FF_DIM), acc_down.reshape(STAGES, LAYERS, FF_DIM, D_MODEL), acc_out)
```

```python
import functools

import jax
import jax.numpy as jnp
from jax import lax
from jax.experimental import pallas as pl
from jax.experimental.pallas import tpu as pltpu
from jax.sharding import PartitionSpec as P

NORM_EPS = 1e-6
FB = 1024
WB = 256
VB = 512
RING = 3
GELU_C = 0.7978845608028654
GELU_K = 0.044715
VMEM_LIMIT = 67_000_000
MESH = pl.DeviceIdType.MESH
F32 = jnp.float32
BF16 = jnp.bfloat16
ANY = pl.BlockSpec(memory_space=pl.ANY)


def dot_nn(a, b):
    return jnp.dot(a, b, preferred_element_type=F32)


def dot_nt(a, b):
    return lax.dot_general(a, b, (((1,), (1,)), ((), ())), preferred_element_type=F32)


def dot_tn(a, b):
    return lax.dot_general(a, b, (((0,), (0,)), ((), ())), preferred_element_type=F32)


def gelu_and_slope(a):
    sq = a * a
    t = jnp.tanh(a * (GELU_C + (GELU_C * GELU_K) * sq))
    cdf = 0.5 + 0.5 * t
    slope = cdf + a * ((0.5 - 0.5 * (t * t)) * (GELU_C + (3.0 * GELU_C * GELU_K) * sq))
    return a * cdf, slope


def params(collective_id=None, **more):
    return pltpu.CompilerParams(
        vmem_limit_bytes=VMEM_LIMIT,
        collective_id=collective_id,
        has_side_effects=collective_id is not None,
        **more,
    )


def cost(flops, bytes_accessed):
    return pl.CostEstimate(flops=int(flops), bytes_accessed=int(bytes_accessed), transcendentals=0)


def fwd_kernel(n_stage, n_micro, n_tile, x_ref, g_ref, w1_ref, w2_ref, hin_ref, hinp_ref, hfin_ref, gp_ref, u_ref,
               recv, obuf, norm, acc, w1b, w2b, gpb, ub,
               x_sem, w1_sem, w2_sem, gp_sem, u_sem, hs_sem, fin_sem, send_sem, recv_sem, psend_sem, precv_sem, bsend_sem, frecv_sem):
    stage = lax.axis_index('stage')
    dp = lax.axis_index('dp')
    last = n_stage - 1
    n_rows = recv.shape[1]

    barrier = pltpu.get_barrier_semaphore()
    for step in range(1, n_stage):
        pl.semaphore_signal(barrier, inc=1, device_id={'stage': lax.rem(stage + step, n_stage)}, device_id_type=MESH)
    pl.semaphore_signal(barrier, inc=1, device_id={'dp': 1 - dp}, device_id_type=MESH)

    def x_copy(m):
        return pltpu.make_async_copy(x_ref.at[m], recv.at[m], x_sem.at[m])

    def w1_copy(j):
        return pltpu.make_async_copy(w1_ref.at[:, pl.ds(pl.multiple_of(j * FB, FB), FB)], w1b.at[j], w1_sem.at[j])

    def w2_copy(q):
        slot = lax.rem(q, RING)
        j = lax.rem(q, n_tile)
        return pltpu.make_async_copy(w2_ref.at[pl.ds(pl.multiple_of(j * FB, FB), FB), :], w2b.at[slot], w2_sem.at[slot])

    def gp_copy(m, j, slot):
        return pltpu.make_async_copy(gpb.at[slot], gp_ref.at[m, j], gp_sem.at[slot])

    def u_copy(m, j, slot):
        return pltpu.make_async_copy(ub.at[slot], u_ref.at[j, m], u_sem.at[slot])

    def save_copy(m):
        return pltpu.make_async_copy(recv.at[m], hin_ref.at[m], hs_sem.at[m])

    def peer_copy(m):
        return pltpu.make_async_remote_copy(recv.at[m], hinp_ref.at[m], psend_sem.at[m], precv_sem.at[m],
                                            device_id={'dp': 1 - dp}, device_id_type=MESH)

    def next_copy(m):
        return pltpu.make_async_remote_copy(obuf.at[m], recv.at[m], send_sem.at[m], recv_sem.at[m],
                                            device_id={'stage': lax.rem(stage + 1, n_stage)}, device_id_type=MESH)

    def fin_copy(m):
        return pltpu.make_async_copy(obuf.at[m], hfin_ref.at[m], fin_sem.at[m])

    def bcast_copy(m, k):
        return pltpu.make_async_remote_copy(obuf.at[m], hfin_ref.at[m], bsend_sem.at[m, k], frecv_sem.at[m],
                                            device_id={'stage': k}, device_id_type=MESH)

    w1_copy(0).start()
    w2_copy(0).start()

    @pl.when(stage == 0)
    def _():
        for m in range(n_micro):
            x_copy(m).start()

    for j in range(1, n_tile):
        w1_copy(j).start()
    w2_copy(1).start()

    pl.semaphore_wait(barrier, n_stage)

    def front(m, j):
        q = m * n_tile + j
        slot = lax.rem(q, 2)

        @pl.when(m == 0)
        def _():
            w1_copy(j).wait()

        @pl.when(q >= 2)
        def _():
            gp_copy(m, j, slot).wait()
            u_copy(m, j, slot).wait()

    def micro(m, _):
        @pl.when(stage == 0)
        def _():
            x_copy(m).wait()

        @pl.when(stage > 0)
        def _():
            next_copy(m).wait_recv()

        save_copy(m).start()
        peer_copy(m).start()

        def norm_rows(i, _):
            rows = pl.ds(pl.multiple_of(i * 32, 32), 32)
            r = recv[m, rows, :].astype(F32)
            inv = lax.rsqrt(jnp.mean(r * r, axis=-1, keepdims=True) + NORM_EPS)
            norm[rows, :] = (r * inv * g_ref[...]).astype(BF16)
            return 0

        lax.fori_loop(0, n_rows // 32, norm_rows, 0)

        front(m, 0)
        q0 = m * n_tile
        s0 = lax.rem(q0, 2)
        u, slope = gelu_and_slope(dot_nn(norm[...], w1b[0]))
        gpb[s0] = slope
        ub[s0] = u.astype(BF16)
        gp_copy(m, 0, s0).start()
        u_copy(m, 0, s0).start()
        acc[...] = recv[m].astype(F32)

        def tile(j, _):
            front(m, j)
            q = m * n_tile + j
            slot = lax.rem(q, 2)
            prev = lax.rem(q + 1, 2)
            w2_copy(q - 1).wait()

            @pl.when(q + 1 < n_micro * n_tile)
            def _():
                w2_copy(q + 1).start()

            ring = lax.rem(q - 1, RING)
            acc[...] += dot_nn(ub[prev], w2b[ring])
            u, slope = gelu_and_slope(dot_nn(norm[...], w1b[j]))
            gpb[slot] = slope
            ub[slot] = u.astype(BF16)
            gp_copy(m, j, slot).start()
            u_copy(m, j, slot).start()
            return 0

        lax.fori_loop(1, n_tile, tile, 0)

        q = m * n_tile + n_tile - 1
        w2_copy(q).wait()

        @pl.when(m < n_micro - 1)
        def _():
            w2_copy(q + 2).start()

        obuf[m] = (acc[...] + dot_nn(ub[lax.rem(q, 2)], w2b[lax.rem(q, RING)])).astype(BF16)

        @pl.when(stage < last)
        def _():
            next_copy(m).start()

        @pl.when(stage == last)
        def _():
            fin_copy(m).start()
            for k in range(last):
                bcast_copy(m, k).start()

        return 0

    lax.fori_loop(0, n_micro, micro, 0)

    end = n_micro * n_tile
    for q in (end - 2, end - 1):
        gp_copy(q // n_tile, q % n_tile, q % 2).wait()
        u_copy(q // n_tile, q % n_tile, q % 2).wait()
    for m in range(n_micro):
        save_copy(m).wait()
        peer_copy(m).wait()

        @pl.when(stage < last)
        def _():
            next_copy(m).wait_send()
            bcast_copy(m, 0).wait_recv()

        @pl.when(stage == last)
        def _():
            fin_copy(m).wait()
            for k in range(last):
                bcast_copy(m, k).wait_send()


def forward(n_stage, x, gain, w1, w2):
    n_micro, n_tok, d = x.shape
    f = w1.shape[1]
    n_tile = f // FB
    dma = pltpu.SemaphoreType.DMA
    act = jax.ShapeDtypeStruct(x.shape, BF16)
    return pl.pallas_call(
        functools.partial(fwd_kernel, n_stage, n_micro, n_tile),
        out_shape=(act, act, act,
                   jax.ShapeDtypeStruct((n_micro, n_tile, n_tok, FB), F32),
                   jax.ShapeDtypeStruct((n_tile, n_micro, n_tok, FB), BF16)),
        in_specs=[ANY, pl.BlockSpec(memory_space=pltpu.VMEM), ANY, ANY],
        out_specs=(ANY,) * 5,
        scratch_shapes=[
            pltpu.VMEM((n_micro, n_tok, d), BF16),
            pltpu.VMEM((n_micro, n_tok, d), BF16),
            pltpu.VMEM((n_tok, d), BF16),
            pltpu.VMEM((n_tok, d), F32),
            pltpu.VMEM((n_tile, d, FB), BF16),
            pltpu.VMEM((RING, FB, d), BF16),
            pltpu.VMEM((2, n_tok, FB), F32),
            pltpu.VMEM((2, n_tok, FB), BF16),
            dma((n_micro,)), dma((n_tile,)), dma((RING,)), dma((2,)), dma((2,)), dma((n_micro,)), dma((n_micro,)),
            dma((n_micro,)), dma((n_micro,)), dma((n_micro,)), dma((n_micro,)), dma((n_micro, n_stage - 1)), dma((n_micro,)),
        ],
        compiler_params=params(0),
        cost_estimate=cost(4 * n_micro * n_tok * d * f, 4 * d * f * (1 + n_micro)),
        name='forward',
    )(x, gain, w1, w2)


def bwd_kernel(n_stage, n_micro, n_tile, top_ref, hin_ref, g_ref, w1_ref, w2_ref, gp_ref, dyin_ref, dyp_ref, da_ref, gx_ref, dg_ref,
               recv, obuf, hbuf, acc, xbuf, w1b, w2b, gpb, dab,
               t_sem, w1_sem, w2_sem, gp_sem, da_sem, h_sem, hs_sem, x_sem, send_sem, recv_sem, psend_sem, precv_sem):
    stage = lax.axis_index('stage')
    dp = lax.axis_index('dp')
    last = n_stage - 1
    n_rows = recv.shape[1]
    total = n_micro * n_tile

    barrier = pltpu.get_barrier_semaphore()
    pl.semaphore_signal(barrier, inc=1, device_id={'dp': 1 - dp}, device_id_type=MESH)

    @pl.when(stage > 0)
    def _():
        pl.semaphore_signal(barrier, inc=1, device_id={'stage': stage - 1}, device_id_type=MESH)

    @pl.when(stage < last)
    def _():
        pl.semaphore_signal(barrier, inc=1, device_id={'stage': stage + 1}, device_id_type=MESH)

    def top_copy(m):
        return pltpu.make_async_copy(top_ref.at[m], recv.at[m], t_sem.at[m])

    def w2_copy(j):
        return pltpu.make_async_copy(w2_ref.at[pl.ds(pl.multiple_of(j * FB, FB), FB), :], w2b.at[j], w2_sem.at[j])

    def w1_copy(q):
        slot = lax.rem(q, RING)
        j = lax.rem(q, n_tile)
        return pltpu.make_async_copy(w1_ref.at[:, pl.ds(pl.multiple_of(j * FB, FB), FB)], w1b.at[slot], w1_sem.at[slot])

    def gp_copy(q):
        slot = lax.rem(q, 2)
        return pltpu.make_async_copy(gp_ref.at[lax.div(q, n_tile), lax.rem(q, n_tile)], gpb.at[slot], gp_sem.at[slot])

    def da_copy(m, j, slot):
        return pltpu.make_async_copy(dab.at[slot], da_ref.at[j, m], da_sem.at[slot])

    def h_copy(m):
        return pltpu.make_async_copy(hin_ref.at[m], hbuf, h_sem)

    def save_copy(m):
        return pltpu.make_async_copy(recv.at[m], dyin_ref.at[m], hs_sem.at[m])

    def peer_copy(m):
        return pltpu.make_async_remote_copy(recv.at[m], dyp_ref.at[m], psend_sem.at[m], precv_sem.at[m],
                                            device_id={'dp': 1 - dp}, device_id_type=MESH)

    def next_copy(m):
        slot = lax.rem(m, 2)
        return pltpu.make_async_remote_copy(obuf.at[slot], recv.at[m], send_sem.at[slot], recv_sem.at[m],
                                            device_id={'stage': lax.rem(stage + last, n_stage)}, device_id_type=MESH)

    def x_copy(m):
        return pltpu.make_async_copy(xbuf, gx_ref.at[m], x_sem)

    @pl.when(stage == last)
    def _():
        for m in range(n_micro):
            top_copy(m).start()

    gp_copy(0).start()
    w2_copy(0).start()
    w1_copy(0).start()
    gp_copy(1).start()
    for j in range(1, n_tile):
        w2_copy(j).start()
    w1_copy(1).start()
    dg_ref[...] = jnp.zeros_like(dg_ref)

    def front(m, j):
        q = m * n_tile + j
        slot = lax.rem(q, 2)

        @pl.when(m == 0)
        def _():
            w2_copy(j).wait()

        @pl.when(q >= 2)
        def _():
            da_copy(m, j, slot).wait()

        gp_copy(q).wait()

    def micro(m, _):
        @pl.when(stage == last)
        def _():
            top_copy(m).wait()

        @pl.when(stage < last)
        def _():
            next_copy(m).wait_recv()

        save_copy(m).start()
        h_copy(m).start()

        front(m, 0)
        q0 = m * n_tile
        s0 = lax.rem(q0, 2)
        dab[s0] = (gpb[s0] * dot_nt(recv[m], w2b[0])).astype(BF16)
        da_copy(m, 0, s0).start()
        gp_copy(q0 + 2).start()
        acc[...] = jnp.zeros_like(acc)

        def tile(j, _):
            front(m, j)
            q = m * n_tile + j
            slot = lax.rem(q, 2)
            prev = lax.rem(q + 1, 2)
            w1_copy(q - 1).wait()

            @pl.when(q + 1 < total)
            def _():
                w1_copy(q + 1).start()

            acc[...] += dot_nt(dab[prev], w1b[lax.rem(q - 1, RING)])
            dab[slot] = (gpb[slot] * dot_nt(recv[m], w2b[j])).astype(BF16)
            da_copy(m, j, slot).start()

            @pl.when(q + 2 < total)
            def _():
                gp_copy(q + 2).start()

            return 0

        lax.fori_loop(1, n_tile, tile, 0)

        q = m * n_tile + n_tile - 1
        w1_copy(q).wait()

        @pl.when(m < n_micro - 1)
        def _():
            w1_copy(q + 2).start()

        acc[...] += dot_nt(dab[lax.rem(q, 2)], w1b[lax.rem(q, RING)])
        h_copy(m).wait()

        @pl.when(m == 0)
        def _():
            pl.semaphore_wait(barrier, 1 + jnp.minimum(stage, 1) + jnp.minimum(last - stage, 1))

        peer_copy(m).start()

        @pl.when((stage > 0) & (m >= 2))
        def _():
            next_copy(m).wait_send()

        @pl.when((stage == 0) & (m >= 1))
        def _():
            x_copy(m).wait()

        oslot = lax.rem(m, 2)

        def norm_rows(i, dg):
            rows = pl.ds(pl.multiple_of(i * 16, 16), 16)
            r = hbuf[rows, :].astype(F32)
            inv = lax.rsqrt(jnp.mean(r * r, axis=-1, keepdims=True) + NORM_EPS)
            hat = r * inv
            dn = acc[rows, :]
            dg = dg + jnp.sum((dn * hat).reshape(2, 8, dn.shape[1]), axis=0)
            dgn = dn * g_ref[...]
            grad = recv[m, rows, :].astype(F32) + inv * (dgn - hat * jnp.mean(dgn * hat, axis=-1, keepdims=True))
            obuf[oslot, rows, :] = grad.astype(BF16)
            xbuf[rows, :] = grad
            return dg

        dg_ref[...] += lax.fori_loop(0, n_rows // 16, norm_rows, jnp.zeros(dg_ref.shape, F32))

        @pl.when(stage > 0)
        def _():
            next_copy(m).start()

        @pl.when(stage == 0)
        def _():
            x_copy(m).start()

        return 0

    lax.fori_loop(0, n_micro, micro, 0)

    for q in (total - 2, total - 1):
        da_copy(q // n_tile, q % n_tile, q % 2).wait()
    for m in range(n_micro):
        save_copy(m).wait()
        peer_copy(m).wait()

    @pl.when(stage > 0)
    def _():
        next_copy(n_micro - 2).wait_send()
        next_copy(n_micro - 1).wait_send()

    @pl.when(stage == 0)
    def _():
        x_copy(n_micro - 1).wait()


def backward(n_stage, top, hin, gain, w1, w2, gp):
    n_micro, n_tok, d = hin.shape
    f = w1.shape[1]
    n_tile = f // FB
    dma = pltpu.SemaphoreType.DMA
    act = jax.ShapeDtypeStruct(hin.shape, BF16)
    vmem = pl.BlockSpec(memory_space=pltpu.VMEM)
    return pl.pallas_call(
        functools.partial(bwd_kernel, n_stage, n_micro, n_tile),
        out_shape=(act, act,
                   jax.ShapeDtypeStruct((n_tile, n_micro, n_tok, FB), BF16),
                   jax.ShapeDtypeStruct(hin.shape, F32),
                   jax.ShapeDtypeStruct((8, d), F32)),
        in_specs=[ANY, ANY, vmem, ANY, ANY, ANY],
        out_specs=(ANY, ANY, ANY, ANY, vmem),
        scratch_shapes=[
            pltpu.VMEM((n_micro, n_tok, d), BF16),
            pltpu.VMEM((2, n_tok, d), BF16),
            pltpu.VMEM((n_tok, d), BF16),
            pltpu.VMEM((n_tok, d), F32),
            pltpu.VMEM((n_tok, d), F32),
            pltpu.VMEM((RING, d, FB), BF16),
            pltpu.VMEM((n_tile, FB, d), BF16),
            pltpu.VMEM((2, n_tok, FB), F32),
            pltpu.VMEM((2, n_tok, FB), BF16),
            dma((n_micro,)), dma((RING,)), dma((n_tile,)), dma((2,)), dma((2,)), dma, dma((n_micro,)), dma,
            dma((2,)), dma((n_micro,)), dma((n_micro,)), dma((n_micro,)),
        ],
        compiler_params=params(1),
        cost_estimate=cost(4 * n_micro * n_tok * d * f, 4 * d * f * (1 + n_micro)),
        name='backward',
    )(top, hin, gain, w1, w2, gp)


def logits_kernel(base_ref, h_ref, w_ref, lab_ref, z_ref, st_ref, m_s, s_s, t_s):
    i = pl.program_id(0)

    @pl.when(i == 0)
    def _():
        m_s[...] = jnp.full(m_s.shape, -jnp.inf, F32)
        s_s[...] = jnp.zeros(s_s.shape, F32)
        t_s[...] = jnp.zeros(t_s.shape, F32)

    z = dot_nt(h_ref[...], w_ref[...])
    z_ref[0] = z
    lane = lax.broadcasted_iota(jnp.int32, (1, 128), 1) + (base_ref[0] + i * VB)
    cols = [z[:, c:c + 128] for c in range(0, VB, 128)]
    m_old = m_s[...]
    m_new = m_old
    for part in cols:
        m_new = jnp.maximum(m_new, part)
    s_new = s_s[...] * jnp.exp(m_old - m_new)
    t_new = t_s[...]
    lab = lab_ref[...]
    for c, part in enumerate(cols):
        s_new = s_new + jnp.exp(part - m_new)
        t_new = t_new + jnp.where(lab == lane + c * 128, part, 0.0)
    m_s[...] = m_new
    s_s[...] = s_new
    t_s[...] = t_new

    @pl.when(i == pl.num_programs(0) - 1)
    def _():
        m_all = jnp.max(m_s[...], axis=1, keepdims=True)
        s_all = jnp.sum(s_s[...] * jnp.exp(m_s[...] - m_all), axis=1, keepdims=True)
        t_all = jnp.sum(t_s[...], axis=1, keepdims=True)
        col = lax.broadcasted_iota(jnp.int32, m_s.shape, 1)
        packed = jnp.where(col == 0, m_all, jnp.where(col == 1, s_all, t_all))
        st_ref[...] = packed.T[:8]


def logits(base, h, w, lab):
    n_tok, d = h.shape
    n_voc = w.shape[0]
    n_tile = n_voc // VB
    once = pl.Buffered(1)
    return pl.pallas_call(
        logits_kernel,
        out_shape=(jax.ShapeDtypeStruct((n_tile, n_tok, VB), F32), jax.ShapeDtypeStruct((8, n_tok), F32)),
        grid_spec=pltpu.PrefetchScalarGridSpec(
            num_scalar_prefetch=1,
            grid=(n_tile,),
            in_specs=[
                pl.BlockSpec((n_tok, d), lambda i, s: (0, 0), pipeline_mode=once),
                pl.BlockSpec((VB, d), lambda i, s: (i, 0)),
                pl.BlockSpec((n_tok, 128), lambda i, s: (0, 0), pipeline_mode=once),
            ],
            out_specs=(pl.BlockSpec((1, n_tok, VB), lambda i, s: (i, 0, 0)), pl.BlockSpec((8, n_tok), lambda i, s: (0, 0))),
            scratch_shapes=[pltpu.VMEM((n_tok, 128), F32)] * 3,
        ),
        compiler_params=params(),
        cost_estimate=cost(2 * n_tok * d * n_voc, 2 * d * n_voc + 4 * n_tok * n_voc),
        name='logits',
    )(base, h, w, lab)


def dz_of(z, lse, lab, lane, scale):
    parts = []
    for c in range(0, z.shape[1], 128):
        p = jnp.exp(z[:, c:c + 128] - lse)
        hot = jnp.where(lab == lane + c, 1.0, 0.0)
        parts.append(((p - hot) * scale).astype(BF16))
    return jnp.concatenate(parts, axis=1)


def dhid_kernel(scale, base_ref, z_ref, w_ref, lse_ref, lab_ref, dz_ref, dh_ref):
    i = pl.program_id(0)

    @pl.when(i == 0)
    def _():
        dh_ref[...] = jnp.zeros(dh_ref.shape, F32)

    lane = lax.broadcasted_iota(jnp.int32, (1, 128), 1) + (base_ref[0] + i * VB)
    dz = dz_of(z_ref[0], lse_ref[...], lab_ref[...], lane, scale)
    dz_ref[0] = dz
    dh_ref[...] += dot_nn(dz, w_ref[...])


def dhid(scale, half, n_half, base, z, w, lse, lab):
    n_tile, n_tok, _ = z.shape
    rows = n_tok // n_half
    n_voc, d = w.shape
    once = pl.Buffered(1)
    return pl.pallas_call(
        functools.partial(dhid_kernel, scale),
        out_shape=(jax.ShapeDtypeStruct((n_tile, rows, VB), BF16), jax.ShapeDtypeStruct((rows, d), F32)),
        grid_spec=pltpu.PrefetchScalarGridSpec(
            num_scalar_prefetch=1,
            grid=(n_tile,),
            in_specs=[
                pl.BlockSpec((1, rows, VB), lambda i, s: (i, half, 0)),
                pl.BlockSpec((VB, d), lambda i, s: (i, 0)),
                pl.BlockSpec((rows, 128), lambda i, s: (half, 0), pipeline_mode=once),
                pl.BlockSpec((rows, 128), lambda i, s: (half, 0), pipeline_mode=once),
            ],
            out_specs=(pl.BlockSpec((1, rows, VB), lambda i, s: (i, 0, 0)), pl.BlockSpec((rows, d), lambda i, s: (0, 0))),
        ),
        compiler_params=params(),
        cost_estimate=cost(2 * rows * d * n_voc, 2 * d * n_voc + 6 * rows * n_voc),
        name=f'dhid{half}',
    )(base, z, w, lse, lab)


def dwout_kernel(scale, s_ref, w_ref, dz0_ref, dz1_ref, ho_ref, hp_ref, lse_ref, lab_ref, *rest):
    out_ref = rest[-1]
    i = pl.program_id(0)

    @pl.when(i < s_ref[2])
    def _():
        rows = dz0_ref.shape[1]
        zp = dot_nt(hp_ref[...], w_ref[...])
        own = dot_tn(dz0_ref[0], ho_ref[:rows, :]) + dot_tn(dz1_ref[0], ho_ref[rows:, :])
        lane = lax.broadcasted_iota(jnp.int32, (1, 128), 1) + (s_ref[0] + (s_ref[1] + i) * VB)
        dzp = dz_of(zp, lse_ref[...], lab_ref[...], lane, scale)
        out_ref[...] = own + dot_tn(dzp, hp_ref[...])


def dwout(scale, n_step, scalars, w, dz0, dz1, ho, hp, lse, lab, out=None):
    n_voc, d = w.shape
    n_tok = ho.shape[0]
    rows = dz0.shape[1]
    once = pl.Buffered(1)

    def at(i, s):
        return jnp.minimum(s[1] + jnp.minimum(i, jnp.maximum(s[2] - 1, 0)), n_voc // VB - 1)

    more = [] if out is None else [out]
    return pl.pallas_call(
        functools.partial(dwout_kernel, scale),
        out_shape=jax.ShapeDtypeStruct((n_voc, d), F32),
        grid_spec=pltpu.PrefetchScalarGridSpec(
            num_scalar_prefetch=1,
            grid=(n_step,),
            in_specs=[
                pl.BlockSpec((VB, d), lambda i, s: (at(i, s), 0)),
                pl.BlockSpec((1, rows, VB), lambda i, s: (at(i, s), 0, 0)),
                pl.BlockSpec((1, rows, VB), lambda i, s: (at(i, s), 0, 0)),
                pl.BlockSpec((n_tok, d), lambda i, s: (0, 0), pipeline_mode=once),
                pl.BlockSpec((n_tok, d), lambda i, s: (0, 0), pipeline_mode=once),
                pl.BlockSpec((n_tok, 128), lambda i, s: (0, 0), pipeline_mode=once),
                pl.BlockSpec((n_tok, 128), lambda i, s: (0, 0), pipeline_mode=once),
            ] + [ANY] * len(more),
            out_specs=pl.BlockSpec((VB, d), lambda i, s: (at(i, s), 0)),
        ),
        input_output_aliases={} if out is None else {8: 0},
        compiler_params=params(),
        cost_estimate=cost(6 * n_tok * d * n_step * VB, (2 * d + 4 * d + 2 * n_tok) * n_step * VB),
        name='dwout_first' if out is None else 'dwout_rest',
    )(scalars, w, dz0, dz1, ho, hp, lse, lab, *more)


def wgrad_kernel(g_ref, ho_ref, hp_ref, dyo_ref, dyp_ref, w1_ref, w2_ref, u_ref, da_ref, dw1_ref, dw2_ref, nt_s, np_s):
    i = pl.program_id(0)
    n_tok = ho_ref.shape[0]

    @pl.when(i == 0)
    def _():
        def prep(src, base, keep):
            def rows_of(k, _):
                rows = pl.ds(pl.multiple_of(k * 128, 128), 128)
                r = src[rows, :].astype(F32)
                inv = lax.rsqrt(jnp.mean(r * r, axis=-1, keepdims=True) + NORM_EPS)
                n = (r * inv * g_ref[...]).astype(BF16)
                if keep:
                    np_s[rows, :] = n
                nt_s[:, pl.ds(pl.multiple_of(base + k * 128, 128), 128)] = n.T
                return 0

            lax.fori_loop(0, n_tok // 128, rows_of, 0)

        prep(ho_ref, 0, False)
        prep(hp_ref, n_tok, True)

    n_col = w1_ref.shape[1]
    a = dot_nn(np_s[...], w1_ref[...])
    dact = dot_nt(dyp_ref[...], w2_ref[...])
    u_own = u_ref[0].reshape(n_tok, n_col)
    da_own = da_ref[0].reshape(n_tok, n_col)
    dw2_own = dot_tn(u_own, dyo_ref[...])
    u, slope = gelu_and_slope(a)
    da = (slope * dact).astype(BF16)
    dw1_ref[...] = dot_nn(nt_s[:, :n_tok], da_own) + dot_nn(nt_s[:, n_tok:], da)
    dw2_ref[...] = dw2_own + dot_tn(u.astype(BF16), dyp_ref[...])


def wgrad(gain, ho, hp, dyo, dyp, w1, w2, u, da):
    n_tok, d = ho.shape
    f = w1.shape[1]
    per = FB // WB
    n_micro, n_row = u.shape[1:3]
    once = pl.Buffered(1)
    full = pl.BlockSpec((n_tok, d), lambda i: (0, 0), pipeline_mode=once)
    act = pl.BlockSpec((1, n_micro, n_row, WB), lambda i: (i // per, 0, 0, i % per))
    return pl.pallas_call(
        wgrad_kernel,
        out_shape=(jax.ShapeDtypeStruct((d, f), F32), jax.ShapeDtypeStruct((f, d), F32)),
        grid=(f // WB,),
        in_specs=[
            pl.BlockSpec((1, d), lambda i: (0, 0), pipeline_mode=once),
            full, full, full, full,
            pl.BlockSpec((d, WB), lambda i: (0, i)),
            pl.BlockSpec((WB, d), lambda i: (i, 0)),
            act, act,
        ],
        out_specs=(pl.BlockSpec((d, WB), lambda i: (0, i)), pl.BlockSpec((WB, d), lambda i: (i, 0))),
        scratch_shapes=[pltpu.VMEM((d, 2 * n_tok), BF16), pltpu.VMEM((n_tok, d), BF16)],
        compiler_params=params(),
        cost_estimate=cost(12 * n_tok * d * f, 12 * d * f + 4 * n_tok * f),
        name='wgrad',
    )(gain, ho, hp, dyo, dyp, w1, w2, u, da)


FIRST_TILES = (21, 18, 12, 9)


def solution(mesh):
    n_stage = mesh.shape['stage']
    n_dp = mesh.shape['dp']
    swap = [(0, 1), (1, 0)]

    def device_step(x_emb, labels, norm_gain, w_up, w_down, w_out):
        n_micro, n_tok, d = x_emb.shape
        own = n_micro * n_tok
        n_voc = w_out.shape[0]
        n_vtile = n_voc // VB
        stage = lax.axis_index('stage')
        dp = lax.axis_index('dp')
        scale = 1.0 / (own * n_dp)
        gain, w1, w2 = norm_gain[0], w_up[0, 0], w_down[0, 0]
        base = (stage * n_voc).reshape(1).astype(jnp.int32)

        def lanes(v):
            return jnp.broadcast_to(v.reshape(own, 1), (own, 128))

        lab = labels.reshape(own)
        lab_o, lab_p = lanes(lab), lanes(lax.ppermute(lab, 'dp', swap))

        hin, hinp, hfin, gp, u = forward(n_stage, x_emb, gain, w1, w2)
        ho = hfin.reshape(own, d)
        z, stats = logits(base, ho, w_out, lab_o)
        hp = lax.ppermute(ho, 'dp', swap)

        every = lax.all_gather(stats, ('dp', 'stage')).reshape(n_dp, n_stage, 8, own)
        top = jnp.max(every[:, :, 0], axis=1)
        lse = top + jnp.log(jnp.sum(every[:, :, 1] * jnp.exp(every[:, :, 0] - top[:, None]), axis=1))
        loss = jnp.sum(lse - jnp.sum(every[:, :, 2], axis=1)) * scale
        lse_o = lanes(lax.dynamic_index_in_dim(lse, dp, 0, keepdims=False))
        lse_p = lanes(lax.dynamic_index_in_dim(lse, 1 - dp, 0, keepdims=False))

        dzs, tops = [], []
        for half in range(2):
            dz, dh = dhid(scale, half, 2, base, z, w_out, lse_o, lab_o)
            dh = dh + lax.ppermute(dh, 'stage', [(0, 1), (2, 3)])
            dh = dh + lax.ppermute(dh, 'stage', [(1, 3)])
            dzs.append(dz)
            tops.append(dh.astype(BF16))
        dtop = jnp.concatenate(tops, axis=0).reshape(n_micro, n_tok, d)

        first = jnp.asarray(FIRST_TILES, jnp.int32)[stage].reshape(1)
        s_first = jnp.concatenate([base, jnp.zeros((1,), jnp.int32), first])
        s_rest = jnp.concatenate([base, first, n_vtile - first])
        head = (w_out, dzs[0], dzs[1], ho, hp, lse_p, lab_p)
        gw = dwout(scale, max(FIRST_TILES), s_first, *head)

        dtop, gw = lax.optimization_barrier((dtop, gw))
        dyin, dyp, da, gx, dg = backward(n_stage, dtop, hin, gain, w1, w2, gp)
        gw, dyin = lax.optimization_barrier((gw, dyin))
        gw = dwout(scale, n_vtile - min(FIRST_TILES), s_rest, *head, out=gw)

        gw, gx, dg, dyin = lax.optimization_barrier((gw, gx, dg, dyin))
        dw1, dw2 = wgrad(gain, hin.reshape(own, d), hinp.reshape(own, d), dyin.reshape(own, d), dyp.reshape(own, d), w1, w2, u, da)

        dg = jnp.sum(dg, axis=0)
        dg = dg + lax.ppermute(dg, 'dp', swap)
        width = d // n_stage
        grad_x = jnp.where(stage == 0, gx[:, :, :width], 0.0)
        for k in range(1, n_stage):
            grad_x = grad_x + lax.ppermute(gx[:, :, k * width:(k + 1) * width], 'stage', [(0, k)])
        return loss.reshape(1), grad_x, dg.reshape(1, 1, d), dw1[None, None], dw2[None, None], gw

    tok_spec = ('pod', 'dp')
    stage_spec = ('pod', 'stage')
    in_specs = (P(None, tok_spec, None), P(None, tok_spec), P(stage_spec, None, None), P(stage_spec, None, None, None), P(stage_spec, None, None, None), P(stage_spec, None))
    out_specs = (P('pod'), P(None, tok_spec, 'stage'), P(stage_spec, None, None), P(stage_spec, None, None, None), P(stage_spec, None, None, None), P(stage_spec, None))
    return jax.shard_map(device_step, mesh=mesh, in_specs=in_specs, out_specs=out_specs, check_vma=False)
```

```python
import functools

import jax
import jax.numpy as jnp
from jax import lax
from jax.experimental import pallas as pl
from jax.experimental.pallas import tpu as pltpu
from jax.sharding import PartitionSpec as P


NORM_EPS = 1e-6
FB = 512
WB = 256
VB = 512
RING = 6
LANES = 128
ROWS = 32
GELU_C = 0.7978845608028654
GELU_K = 0.044715
VMEM_LIMIT = 67_000_000
MESH = pl.DeviceIdType.MESH
F32 = jnp.float32
BF16 = jnp.bfloat16
ANY = pl.BlockSpec(memory_space=pl.ANY)


def dot_nn(a, b):
    return jnp.dot(a[...], b[...], preferred_element_type=F32)


def dot_nt(a, b):
    return lax.dot_general(a[...], b[...], (((1,), (1,)), ((), ())), preferred_element_type=F32)


def dot_tn(a, b):
    return lax.dot_general(a[...], b[...], (((0,), (0,)), ((), ())), preferred_element_type=F32)


def gelu_and_slope(a):
    sq = a * a
    t = jnp.tanh(a * (GELU_C + (GELU_C * GELU_K) * sq))
    cdf = 0.5 + 0.5 * t
    slope = cdf + a * ((0.5 - 0.5 * (t * t)) * (GELU_C + (3.0 * GELU_C * GELU_K) * sq))
    return a * cdf, slope


def home(*_):
    return 0, 0


def params(collective_id=None, **more):
    return pltpu.CompilerParams(
        vmem_limit_bytes=VMEM_LIMIT,
        collective_id=collective_id,
        has_side_effects=collective_id is not None,
        **more,
    )


def cost(flops, bytes_accessed):
    return pl.CostEstimate(flops=int(flops), bytes_accessed=int(bytes_accessed), transcendentals=0)


def fwd_kernel(n_stage, n_micro, n_tile, x_ref, g_ref, w1_ref, w2_ref, hin_ref, hinp_ref, hfin_ref, gp_ref, u_ref,
               recv, obuf, norm, acc, w1b, w2b, gpb, uob, ua, ub,
               x_sem, w1_sem, w2_sem, gp_sem, u_sem, hs_sem, fin_sem, send_sem, recv_sem, psend_sem, precv_sem, bsend_sem, frecv_sem):
    stage = lax.axis_index('stage')
    dp = lax.axis_index('dp')
    last = n_stage - 1
    n_rows = recv.shape[1]
    total = n_micro * n_tile
    n_pair = n_tile // 2

    barrier = pltpu.get_barrier_semaphore()
    for step in range(1, n_stage):
        pl.semaphore_signal(barrier, inc=1, device_id={'stage': lax.rem(stage + step, n_stage)}, device_id_type=MESH)
    pl.semaphore_signal(barrier, inc=1, device_id={'dp': 1 - dp}, device_id_type=MESH)

    def x_copy(m):
        return pltpu.make_async_copy(x_ref.at[m], recv.at[m], x_sem.at[m])

    def w1_copy(j):
        return pltpu.make_async_copy(w1_ref.at[:, pl.ds(pl.multiple_of(j * FB, FB), FB)], w1b.at[j], w1_sem.at[j])

    def w2_copy(q):
        slot = lax.rem(q, RING)
        j = lax.rem(q, n_tile)
        return pltpu.make_async_copy(w2_ref.at[pl.ds(pl.multiple_of(j * FB, FB), FB), :], w2b.at[slot], w2_sem.at[slot])

    def out_copies(m, j, slot, side):
        return (pltpu.make_async_copy(gpb.at[slot, side], gp_ref.at[m, j], gp_sem.at[slot, side]),
                pltpu.make_async_copy(uob.at[slot, side], u_ref.at[j, m], u_sem.at[slot, side]))

    def save_copy(m):
        return pltpu.make_async_copy(recv.at[m], hin_ref.at[m], hs_sem.at[m])

    def peer_copy(m):
        return pltpu.make_async_remote_copy(recv.at[m], hinp_ref.at[m], psend_sem.at[m], precv_sem.at[m],
                                            device_id={'dp': 1 - dp}, device_id_type=MESH)

    def next_copy(m):
        return pltpu.make_async_remote_copy(obuf.at[m], recv.at[m], send_sem.at[m], recv_sem.at[m],
                                            device_id={'stage': lax.rem(stage + 1, n_stage)}, device_id_type=MESH)

    def fin_copy(m):
        return pltpu.make_async_copy(obuf.at[m], hfin_ref.at[m], fin_sem.at[m])

    def bcast_copy(m, k):
        return pltpu.make_async_remote_copy(obuf.at[m], hfin_ref.at[m], bsend_sem.at[m, k], frecv_sem.at[m],
                                            device_id={'stage': k}, device_id_type=MESH)

    def relay_copy(m):
        return pltpu.make_async_remote_copy(hfin_ref.at[m], hfin_ref.at[m], bsend_sem.at[m, 0], frecv_sem.at[m],
                                            device_id={'stage': 0}, device_id_type=MESH)

    w1_copy(0).start()
    w1_copy(1).start()
    w2_copy(0).start()

    @pl.when(stage == 0)
    def _():
        for m in range(n_micro):
            x_copy(m).start()

    for j in range(2, n_tile):
        w1_copy(j).start()
        if j < RING - 1:
            w2_copy(j - 1).start()
    pl.semaphore_wait(barrier, n_stage)

    def ahead(m, j):
        @pl.when(m == 0)
        def _():
            w1_copy(j).wait()

    def refill(q):
        w2_copy(q).wait()

        @pl.when(q + RING - 2 < total)
        def _():
            w2_copy(q + RING - 2).start()

    def hidden(j, slot, side, keep):
        u, slope = gelu_and_slope(dot_nn(norm, w1b[j]))
        gpb[slot, side] = slope
        u = u.astype(BF16)
        uob[slot, side] = u
        keep[...] = u

    def free(slot, side):
        for copy in out_copies(0, 0, slot, side):
            copy.wait()

    def put(m, j, slot, side):
        for copy in out_copies(m, j, slot, side):
            copy.start()

    @pl.loop(0, n_micro)
    def _(m):
        @pl.when(stage == 0)
        def _():
            x_copy(m).wait()

        @pl.when(stage > 0)
        def _():
            next_copy(m).wait_recv()

        save_copy(m).start()
        peer_copy(m).start()

        @pl.loop(0, n_rows, step=ROWS)
        def _(i):
            rows = pl.ds(pl.multiple_of(i, ROWS), ROWS)
            r = recv[m, rows, :].astype(F32)
            inv = lax.rsqrt(jnp.mean(r * r, axis=-1, keepdims=True) + NORM_EPS)
            norm[rows, :] = (r * inv * g_ref[...]).astype(BF16)
            acc[rows, :] = r

        k0 = m * n_pair
        ahead(m, 0)

        @pl.when(k0 >= 2)
        def _():
            free(lax.rem(k0, 2), 0)

        hidden(0, lax.rem(k0, 2), 0, ua)
        put(m, 0, lax.rem(k0, 2), 0)

        @pl.loop(1, n_pair)
        def _(k):
            slot = lax.rem(k0 + k, 2)
            j = 2 * k
            q = m * n_tile + j
            ahead(m, j - 1)
            ahead(m, j)
            refill(q - 2)
            refill(q - 1)

            @pl.when(k0 + k >= 2)
            def _():
                free(slot, 0)

            @pl.when(k0 + k >= 3)
            def _():
                free(slot, 1)

            hidden(j - 1, slot, 1, ub)
            acc[...] += dot_nn(ua, w2b[lax.rem(q - 2, RING)])
            hidden(j, slot, 0, ua)
            acc[...] += dot_nn(ub, w2b[lax.rem(q - 1, RING)])
            put(m, j - 1, slot, 1)
            put(m, j, slot, 0)

        slot = lax.rem(k0 + n_pair, 2)
        q = m * n_tile + n_tile - 1
        ahead(m, n_tile - 1)
        refill(q - 1)
        refill(q)

        @pl.when(k0 + n_pair >= 3)
        def _():
            free(slot, 1)

        hidden(n_tile - 1, slot, 1, ub)
        acc[...] += dot_nn(ua, w2b[lax.rem(q - 1, RING)])
        obuf[m] = (acc[...] + dot_nn(ub, w2b[lax.rem(q, RING)])).astype(BF16)

        @pl.when(stage < last)
        def _():
            next_copy(m).start()

        @pl.when(stage == last)
        def _():
            for k in range(last - 1, 0, -1):
                bcast_copy(m, k).start()
            fin_copy(m).start()

        put(m, n_tile - 1, slot, 1)

    for side in range(2):
        for slot in range(2):
            free(slot, side)

    @pl.when(stage < last)
    def _():
        for m in range(n_micro):
            bcast_copy(m, 1).wait_recv()

            @pl.when(stage == 1)
            def _():
                relay_copy(m).start()

    for m in range(n_micro):
        save_copy(m).wait()
        peer_copy(m).wait()

        @pl.when(stage < last)
        def _():
            next_copy(m).wait_send()

        @pl.when(stage == 1)
        def _():
            relay_copy(m).wait_send()

        @pl.when(stage == last)
        def _():
            fin_copy(m).wait()
            for k in range(1, last):
                bcast_copy(m, k).wait_send()


def forward(n_stage, x, gain, w1, w2):
    n_micro, n_tok, d = x.shape
    f = w1.shape[1]
    n_tile = f // FB
    dma = pltpu.SemaphoreType.DMA
    act = jax.ShapeDtypeStruct(x.shape, BF16)
    return pl.pallas_call(
        functools.partial(fwd_kernel, n_stage, n_micro, n_tile),
        out_shape=(act, act, act,
                   jax.ShapeDtypeStruct((n_micro, n_tile, n_tok, FB), F32),
                   jax.ShapeDtypeStruct((n_tile, n_micro, n_tok, FB), BF16)),
        in_specs=[ANY, pl.BlockSpec(memory_space=pltpu.VMEM), ANY, ANY],
        out_specs=(ANY,) * 5,
        scratch_shapes=[
            pltpu.VMEM((n_micro, n_tok, d), BF16),
            pltpu.VMEM((n_micro, n_tok, d), BF16),
            pltpu.VMEM((n_tok, d), BF16),
            pltpu.VMEM((n_tok, d), F32),
            pltpu.VMEM((n_tile, d, FB), BF16),
            pltpu.VMEM((RING, FB, d), BF16),
            pltpu.VMEM((2, 2, n_tok, FB), F32),
            pltpu.VMEM((2, 2, n_tok, FB), BF16),
            pltpu.VMEM((n_tok, FB), BF16),
            pltpu.VMEM((n_tok, FB), BF16),
            dma((n_micro,)), dma((n_tile,)), dma((RING,)), dma((2, 2)), dma((2, 2)), dma((n_micro,)), dma((n_micro,)),
            dma((n_micro,)), dma((n_micro,)), dma((n_micro,)), dma((n_micro,)), dma((n_micro, n_stage - 1)), dma((n_micro,)),
        ],
        compiler_params=params(0),
        cost_estimate=cost(4 * n_micro * n_tok * d * f, 4 * d * f * (1 + n_micro)),
        name='forward',
    )(x, gain, w1, w2)


def bwd_kernel(n_stage, n_micro, n_tile, top0_ref, top1_ref, hin_ref, g_ref, w1_ref, w2_ref, gp_ref,
               dyin_ref, dyp_ref, da_ref, gx_ref, dg_ref,
               recv, obuf, hbuf, acc, xbuf, w1b, w2b, gpb, dob, da_a, da_b,
               t_sem, w1_sem, w2_sem, gp_sem, da_sem, h_sem, hs_sem, x_sem, send_sem, recv_sem, psend_sem, precv_sem):
    stage = lax.axis_index('stage')
    dp = lax.axis_index('dp')
    last = n_stage - 1
    n_rows, d = recv.shape[1:]
    total = n_micro * n_tile
    n_pair = n_tile // 2

    barrier = pltpu.get_barrier_semaphore()
    pl.semaphore_signal(barrier, inc=1, device_id={'dp': 1 - dp}, device_id_type=MESH)

    @pl.when(stage > 0)
    def _():
        pl.semaphore_signal(barrier, inc=1, device_id={'stage': stage - 1}, device_id_type=MESH)

    @pl.when(stage < last)
    def _():
        pl.semaphore_signal(barrier, inc=1, device_id={'stage': stage + 1}, device_id_type=MESH)

    def top_copy(m):
        half = n_micro // 2
        top_ref = top0_ref if m < half else top1_ref
        return pltpu.make_async_copy(top_ref.at[m % half], recv.at[m], t_sem.at[m])

    def w2_copy(j):
        return pltpu.make_async_copy(w2_ref.at[pl.ds(pl.multiple_of(j * FB, FB), FB), :], w2b.at[j], w2_sem.at[j])

    def w1_copy(q):
        slot = lax.rem(q, RING)
        j = lax.rem(q, n_tile)
        return pltpu.make_async_copy(w1_ref.at[:, pl.ds(pl.multiple_of(j * FB, FB), FB)], w1b.at[slot], w1_sem.at[slot])

    def gp_copy(q):
        slot = lax.rem(q, 4)
        return pltpu.make_async_copy(gp_ref.at[lax.div(q, n_tile), lax.rem(q, n_tile)], gpb.at[slot], gp_sem.at[slot])

    def da_copy(m, j, slot, side):
        return pltpu.make_async_copy(dob.at[slot, side], da_ref.at[j, m], da_sem.at[slot, side])

    def h_copy(m):
        return pltpu.make_async_copy(hin_ref.at[m], hbuf, h_sem)

    def save_copy(m):
        return pltpu.make_async_copy(recv.at[m], dyin_ref.at[m], hs_sem.at[m])

    def peer_copy(m):
        return pltpu.make_async_remote_copy(recv.at[m], dyp_ref.at[m], psend_sem.at[m], precv_sem.at[m],
                                            device_id={'dp': 1 - dp}, device_id_type=MESH)

    def next_copy(m):
        slot = lax.rem(m, 2)
        return pltpu.make_async_remote_copy(obuf.at[slot], recv.at[m], send_sem.at[slot], recv_sem.at[m],
                                            device_id={'stage': lax.rem(stage + last, n_stage)}, device_id_type=MESH)

    def x_copies(m):
        width = d // n_stage
        return [pltpu.make_async_copy(xbuf.at[:, pl.ds(k * width, width)], gx_ref.at[k, m], x_sem.at[k]) for k in range(n_stage)]

    @pl.when(stage == last)
    def _():
        for m in range(n_micro):
            top_copy(m).start()

    w2_copy(0).start()
    for q in range(4):
        gp_copy(q).start()
    w2_copy(1).start()
    w2_copy(2).start()
    w1_copy(0).start()
    for j in range(3, n_tile):
        w2_copy(j).start()
        if j < RING:
            w1_copy(j - 2).start()
    dg_ref[...] = jnp.zeros_like(dg_ref)

    def ahead(m, j):
        @pl.when(m == 0)
        def _():
            w2_copy(j).wait()

        gp_copy(m * n_tile + j).wait()

    def refill(q):
        w1_copy(q).wait()

        @pl.when(q + RING - 2 < total)
        def _():
            w1_copy(q + RING - 2).start()

    def more_slopes(q):
        @pl.when(q < total)
        def _():
            gp_copy(q).start()

    def hidden(m, j, slot, side, keep):
        dact = dot_nt(w2b[j], recv[m])
        da = (gpb[lax.rem(m * n_tile + j, 4)] * dact.T).astype(BF16)
        dob[slot, side] = da
        keep[...] = da

    def run(m):
        @pl.when(stage == last)
        def _():
            for k in range(n_micro):
                @pl.when(m == k)
                def _():
                    top_copy(k).wait()

        @pl.when(stage < last)
        def _():
            next_copy(m).wait_recv()

        save_copy(m).start()
        h_copy(m).start()

        @pl.when(m == 1)
        def _():
            peer_copy(0).start()

        @pl.when(m > 0)
        def _():
            peer_copy(m).start()

        k0 = m * n_pair
        ahead(m, 0)

        @pl.when(k0 >= 2)
        def _():
            da_copy(m, 0, lax.rem(k0, 2), 0).wait()

        acc[...] = jnp.zeros_like(acc)
        hidden(m, 0, lax.rem(k0, 2), 0, da_a)
        da_copy(m, 0, lax.rem(k0, 2), 0).start()
        more_slopes(m * n_tile + 4)

        @pl.loop(1, n_pair)
        def _(k):
            slot = lax.rem(k0 + k, 2)
            j = 2 * k
            q = m * n_tile + j
            ahead(m, j - 1)
            ahead(m, j)
            refill(q - 2)
            refill(q - 1)

            @pl.when(k0 + k >= 2)
            def _():
                da_copy(m, j, slot, 0).wait()

            @pl.when(k0 + k >= 3)
            def _():
                da_copy(m, j, slot, 1).wait()

            hidden(m, j - 1, slot, 1, da_b)
            acc[...] += dot_nt(w1b[lax.rem(q - 2, RING)], da_a)
            hidden(m, j, slot, 0, da_a)
            acc[...] += dot_nt(w1b[lax.rem(q - 1, RING)], da_b)
            da_copy(m, j - 1, slot, 1).start()
            da_copy(m, j, slot, 0).start()
            more_slopes(q + 3)
            more_slopes(q + 4)

        slot = lax.rem(k0 + n_pair, 2)
        q = m * n_tile + n_tile - 1
        ahead(m, n_tile - 1)
        refill(q - 1)
        refill(q)

        @pl.when(k0 + n_pair >= 3)
        def _():
            da_copy(m, 0, slot, 1).wait()

        hidden(m, n_tile - 1, slot, 1, da_b)
        acc[...] += dot_nt(w1b[lax.rem(q - 1, RING)], da_a)
        acc[...] += dot_nt(w1b[lax.rem(q, RING)], da_b)
        da_copy(m, n_tile - 1, slot, 1).start()
        more_slopes(q + 4)

    def finish(m):
        h_copy(m).wait()

        @pl.when((stage > 0) & (m >= 2))
        def _():
            next_copy(m).wait_send()

        @pl.when((stage == 0) & (m >= 1))
        def _():
            for copy in x_copies(m):
                copy.wait()

        @pl.loop(0, d, step=LANES)
        def _(c):
            cols = pl.ds(pl.multiple_of(c, LANES), LANES)
            xbuf[:, cols] = acc[cols, :].T

        oslot = lax.rem(m, 2)

        def norm_rows(i, dg):
            rows = pl.ds(pl.multiple_of(i * 16, 16), 16)
            r = hbuf[rows, :].astype(F32)
            inv = lax.rsqrt(jnp.mean(r * r, axis=-1, keepdims=True) + NORM_EPS)
            hat = r * inv
            dn = xbuf[rows, :]
            dg = dg + jnp.sum((dn * hat).reshape(2, 8, dn.shape[1]), axis=0)
            dgn = dn * g_ref[...]
            grad = recv[m, rows, :].astype(F32) + inv * (dgn - hat * jnp.mean(dgn * hat, axis=-1, keepdims=True))
            obuf[oslot, rows, :] = grad.astype(BF16)
            xbuf[rows, :] = grad
            return dg

        dg_ref[...] += lax.fori_loop(0, n_rows // 16, norm_rows, jnp.zeros(dg_ref.shape, F32))

        @pl.when(m == 0)
        def _():
            pl.semaphore_wait(barrier, 1 + jnp.minimum(stage, 1) + jnp.minimum(last - stage, 1))

        @pl.when(stage > 0)
        def _():
            next_copy(m).start()

        @pl.when(stage == 0)
        def _():
            for copy in x_copies(m):
                copy.start()

    @pl.loop(0, n_micro + 1)
    def _(m):
        @pl.when(m > 0)
        def _():
            finish(m - 1)

        @pl.when(m < n_micro)
        def _():
            run(m)


    for side in range(2):
        for slot in range(2):
            da_copy(0, 0, slot, side).wait()
    for m in range(n_micro):
        save_copy(m).wait()
        peer_copy(m).wait()

    @pl.when(stage > 0)
    def _():
        next_copy(n_micro - 2).wait_send()
        next_copy(n_micro - 1).wait_send()

    @pl.when(stage == 0)
    def _():
        for copy in x_copies(n_micro - 1):
            copy.wait()


def backward(n_stage, tops, hin, gain, w1, w2, gp):
    n_micro, n_tok, d = hin.shape
    f = w1.shape[1]
    n_tile = f // FB
    dma = pltpu.SemaphoreType.DMA
    act = jax.ShapeDtypeStruct(hin.shape, BF16)
    vmem = pl.BlockSpec(memory_space=pltpu.VMEM)
    return pl.pallas_call(
        functools.partial(bwd_kernel, n_stage, n_micro, n_tile),
        out_shape=(act, act,
                   jax.ShapeDtypeStruct((n_tile, n_micro, n_tok, FB), BF16),
                   jax.ShapeDtypeStruct((n_stage, n_micro, n_tok, d // n_stage), F32),
                   jax.ShapeDtypeStruct((8, d), F32)),
        in_specs=[ANY, ANY, ANY, vmem, ANY, ANY, ANY],
        out_specs=(ANY, ANY, ANY, ANY, vmem),
        scratch_shapes=[
            pltpu.VMEM((n_micro, n_tok, d), BF16),
            pltpu.VMEM((2, n_tok, d), BF16),
            pltpu.VMEM((n_tok, d), BF16),
            pltpu.VMEM((d, n_tok), F32),
            pltpu.VMEM((n_tok, d), F32),
            pltpu.VMEM((RING, d, FB), BF16),
            pltpu.VMEM((n_tile, FB, d), BF16),
            pltpu.VMEM((4, n_tok, FB), F32),
            pltpu.VMEM((2, 2, n_tok, FB), BF16),
            pltpu.VMEM((n_tok, FB), BF16),
            pltpu.VMEM((n_tok, FB), BF16),
            dma((n_micro,)), dma((RING,)), dma((n_tile,)), dma((4,)), dma((2, 2)), dma, dma((n_micro,)), dma((n_stage,)),
            dma((2,)), dma((n_micro,)), dma((n_micro,)), dma((n_micro,)),
        ],
        compiler_params=params(1),
        cost_estimate=cost(4 * n_micro * n_tok * d * f, 4 * d * f * (1 + n_micro)),
        name='backward',
    )(*tops, hin, gain, w1, w2, gp)


def logits_kernel(base_ref, h_ref, w_ref, lab_ref, z_ref, st_ref, m_s, s_s, t_s, zs):
    i = pl.program_id(0)

    @pl.when(i == 0)
    def _():
        m_s[...] = jnp.full(m_s.shape, -jnp.inf, F32)
        s_s[...] = jnp.zeros(s_s.shape, F32)
        t_s[...] = jnp.zeros(t_s.shape, F32)
        zs[...] = jnp.full(zs.shape, -jnp.inf, F32)

    def count(z, first):
        lane = lax.broadcasted_iota(jnp.int32, (1, LANES), 1) + first
        cols = [z[:, c:c + LANES] for c in range(0, VB, LANES)]
        m_old = m_s[...]
        m_new = m_old
        for part in cols:
            m_new = jnp.maximum(m_new, part)
        m_ref = jnp.where(m_new == -jnp.inf, 0.0, m_new)
        s_new = s_s[...] * jnp.exp(m_old - m_ref)
        t_new = t_s[...]
        lab = lab_ref[...]
        for c, part in enumerate(cols):
            s_new = s_new + jnp.exp(part - m_ref)
            t_new = t_new + jnp.where(lab == lane + c * LANES, part, 0.0)
        m_s[...] = m_new
        s_s[...] = s_new
        t_s[...] = t_new

    first = base_ref[0] + i * (2 * VB)
    z_ref[0] = dot_nt(h_ref, w_ref[:VB, :])
    count(zs[...], jnp.where(i == 0, -(1 << 20), first - VB))
    z = dot_nt(h_ref, w_ref[VB:, :])
    z_ref[1] = z
    zs[...] = z
    count(z_ref[0], first)

    @pl.when(i == pl.num_programs(0) - 1)
    def _():
        count(zs[...], first + VB)
        m_all = jnp.max(m_s[...], axis=1, keepdims=True)
        s_all = jnp.sum(s_s[...] * jnp.exp(m_s[...] - m_all), axis=1, keepdims=True)
        t_all = jnp.sum(t_s[...], axis=1, keepdims=True)
        col = lax.broadcasted_iota(jnp.int32, m_s.shape, 1)
        packed = jnp.where(col == 0, m_all, jnp.where(col == 1, s_all, t_all))
        st_ref[...] = packed.T[:8]


def logits(base, h, w, lab):
    n_tok, d = h.shape
    n_voc = w.shape[0]
    n_tile = n_voc // VB
    once = pl.Buffered(1)
    return pl.pallas_call(
        logits_kernel,
        out_shape=(jax.ShapeDtypeStruct((n_tile, n_tok, VB), F32), jax.ShapeDtypeStruct((8, n_tok), F32)),
        grid_spec=pltpu.PrefetchScalarGridSpec(
            num_scalar_prefetch=1,
            grid=(n_tile // 2,),
            in_specs=[
                pl.BlockSpec((n_tok, d), home, pipeline_mode=once),
                pl.BlockSpec((2 * VB, d), lambda i, s: (i, 0)),
                pl.BlockSpec((n_tok, LANES), home, pipeline_mode=once),
            ],
            out_specs=(pl.BlockSpec((2, n_tok, VB), lambda i, s: (i, 0, 0)), pl.BlockSpec((8, n_tok), home)),
            scratch_shapes=[pltpu.VMEM((n_tok, LANES), F32)] * 3 + [pltpu.VMEM((n_tok, VB), F32)],
        ),
        compiler_params=params(),
        cost_estimate=cost(2 * n_tok * d * n_voc, 2 * d * n_voc + 4 * n_tok * n_voc),
        name='logits',
    )(base, h, w, lab)


def dz_of(z, lse, lab, lane, scale):
    parts = []
    for c in range(0, z.shape[1], LANES):
        p = jnp.exp(z[:, c:c + LANES] - lse)
        hot = jnp.where(lab == lane + c, 1.0, 0.0)
        parts.append(((p - hot) * scale).astype(BF16))
    return jnp.concatenate(parts, axis=1)


def dhid_kernel(scale, base_ref, z_ref, wa_ref, wb_ref, wl_ref, lse_ref, lab_ref, dz_ref, dh_ref, dz_a, dz_b):
    i = pl.program_id(0)

    @pl.when(i == 0)
    def _():
        dh_ref[...] = jnp.zeros(dh_ref.shape, F32)
        dz_b[...] = jnp.zeros(dz_b.shape, BF16)

    def turn(k, keep):
        lane = lax.broadcasted_iota(jnp.int32, (1, LANES), 1) + (base_ref[0] + (2 * i + k) * VB)
        dz = dz_of(z_ref[k], lse_ref[...], lab_ref[...], lane, scale)
        dz_ref[k] = dz
        keep[...] = dz

    turn(0, dz_a)
    dh_ref[...] += dot_nn(dz_b, wb_ref)
    turn(1, dz_b)
    dh_ref[...] += dot_nn(dz_a, wa_ref)

    @pl.when(i == pl.num_programs(0) - 1)
    def _():
        dh_ref[...] += dot_nn(dz_b, wl_ref)


def dhid(scale, half, n_half, base, z, w, lse, lab):
    n_tile, n_tok, _ = z.shape
    rows = n_tok // n_half
    n_voc, d = w.shape
    once = pl.Buffered(1)
    return pl.pallas_call(
        functools.partial(dhid_kernel, scale),
        out_shape=(jax.ShapeDtypeStruct((n_tile, rows, VB), BF16), jax.ShapeDtypeStruct((rows, d), F32)),
        grid_spec=pltpu.PrefetchScalarGridSpec(
            num_scalar_prefetch=1,
            grid=(n_tile // 2,),
            in_specs=[
                pl.BlockSpec((2, rows, VB), lambda i, s: (i, half, 0)),
                pl.BlockSpec((VB, d), lambda i, s: (2 * i, 0)),
                pl.BlockSpec((VB, d), lambda i, s: (jnp.maximum(2 * i - 1, 0), 0)),
                pl.BlockSpec((VB, d), lambda i, s: (n_tile - 1, 0), pipeline_mode=once),
                pl.BlockSpec((rows, LANES), lambda i, s: (half, 0), pipeline_mode=once),
                pl.BlockSpec((rows, LANES), lambda i, s: (half, 0), pipeline_mode=once),
            ],
            out_specs=(pl.BlockSpec((2, rows, VB), lambda i, s: (i, 0, 0)), pl.BlockSpec((rows, d), home)),
            scratch_shapes=[pltpu.VMEM((rows, VB), BF16)] * 2,
        ),
        compiler_params=params(),
        cost_estimate=cost(2 * rows * d * n_voc, 2 * d * n_voc + 6 * rows * n_voc),
    )(base, z, w, w, w, lse, lab)


def dwout_kernel(scale, s_ref, w_ref, dz0_ref, dz1_ref, ho_ref, hp_ref, lse_ref, lab_ref, *rest):
    out_ref = rest[-1]
    i = pl.program_id(0)

    @pl.when(i < s_ref[2])
    def _():
        rows = dz0_ref.shape[1]
        zp = dot_nt(hp_ref, w_ref)
        own = dot_tn(dz0_ref[0], ho_ref[:rows, :]) + dot_tn(dz1_ref[0], ho_ref[rows:, :])
        lane = lax.broadcasted_iota(jnp.int32, (1, LANES), 1) + (s_ref[0] + (s_ref[1] + i) * VB)
        dzp = dz_of(zp, lse_ref[...], lab_ref[...], lane, scale)
        out_ref[...] = own + dot_tn(dzp, hp_ref)


def dwout(scale, n_step, scalars, w, dz0, dz1, ho, hp, lse, lab, out=None):
    n_voc, d = w.shape
    n_tok = ho.shape[0]
    rows = dz0.shape[1]
    once = pl.Buffered(1)

    def at(i, s):
        return jnp.minimum(s[1] + jnp.minimum(i, jnp.maximum(s[2] - 1, 0)), n_voc // VB - 1)

    more = [] if out is None else [out]
    return pl.pallas_call(
        functools.partial(dwout_kernel, scale),
        out_shape=jax.ShapeDtypeStruct((n_voc, d), F32),
        grid_spec=pltpu.PrefetchScalarGridSpec(
            num_scalar_prefetch=1,
            grid=(n_step,),
            in_specs=[
                pl.BlockSpec((VB, d), lambda i, s: (at(i, s), 0)),
                pl.BlockSpec((1, rows, VB), lambda i, s: (at(i, s), 0, 0)),
                pl.BlockSpec((1, rows, VB), lambda i, s: (at(i, s), 0, 0)),
                pl.BlockSpec((n_tok, d), home, pipeline_mode=once),
                pl.BlockSpec((n_tok, d), home, pipeline_mode=once),
                pl.BlockSpec((n_tok, LANES), home, pipeline_mode=once),
                pl.BlockSpec((n_tok, LANES), home, pipeline_mode=once),
            ] + [ANY] * len(more),
            out_specs=pl.BlockSpec((VB, d), lambda i, s: (at(i, s), 0)),
        ),
        input_output_aliases={} if out is None else {8: 0},
        compiler_params=params(),
        cost_estimate=cost(6 * n_tok * d * n_step * VB, (2 * d + 4 * d + 2 * n_tok) * n_step * VB),
        name='dwout_first' if out is None else 'dwout_rest',
    )(scalars, w, dz0, dz1, ho, hp, lse, lab, *more)


def wgrad_kernel(g_ref, ho_ref, hp_ref, dyo_ref, dyp_ref, w1_ref, w2_ref, u_ref, da_ref, dw1_ref, dw2_ref, nt_s, np_s):
    i = pl.program_id(0)
    n_tok = ho_ref.shape[0]

    @pl.when(i == 0)
    def _():
        def prep(src, base, keep):
            @pl.loop(0, n_tok, step=LANES)
            def _(k):
                rows = pl.ds(pl.multiple_of(k, LANES), LANES)
                r = src[rows, :].astype(F32)
                inv = lax.rsqrt(jnp.mean(r * r, axis=-1, keepdims=True) + NORM_EPS)
                n = (r * inv * g_ref[...]).astype(BF16)
                if keep:
                    np_s[rows, :] = n
                nt_s[:, pl.ds(pl.multiple_of(base + k, LANES), LANES)] = n.T

        prep(ho_ref, 0, False)
        prep(hp_ref, n_tok, True)

    n_col = w1_ref.shape[1]
    a = dot_nn(np_s, w1_ref)
    dact = dot_nt(dyp_ref, w2_ref)
    u_own = u_ref[0].reshape(n_tok, n_col)
    da_own = da_ref[0].reshape(n_tok, n_col)
    dw2_own = dot_tn(u_own, dyo_ref)
    u, slope = gelu_and_slope(a)
    da = (slope * dact).astype(BF16)
    dw1_ref[...] = dot_nn(nt_s[:, :n_tok], da_own) + dot_nn(nt_s[:, n_tok:], da)
    dw2_ref[...] = dw2_own + dot_tn(u.astype(BF16), dyp_ref)


def wgrad(gain, ho, hp, dyo, dyp, w1, w2, u, da):
    n_tok, d = ho.shape
    f = w1.shape[1]
    per = FB // WB
    n_micro, n_row = u.shape[1:3]
    once = pl.Buffered(1)
    full = pl.BlockSpec((n_tok, d), home, pipeline_mode=once)
    act = pl.BlockSpec((1, n_micro, n_row, WB), lambda i: (i // per, 0, 0, i % per))
    return pl.pallas_call(
        wgrad_kernel,
        out_shape=(jax.ShapeDtypeStruct((d, f), F32), jax.ShapeDtypeStruct((f, d), F32)),
        grid=(f // WB,),
        in_specs=[
            pl.BlockSpec((1, d), home, pipeline_mode=once),
            full, full, full, full,
            pl.BlockSpec((d, WB), lambda i: (0, i)),
            pl.BlockSpec((WB, d), lambda i: (i, 0)),
            act, act,
        ],
        out_specs=(pl.BlockSpec((d, WB), lambda i: (0, i)), pl.BlockSpec((WB, d), lambda i: (i, 0))),
        scratch_shapes=[pltpu.VMEM((d, 2 * n_tok), BF16), pltpu.VMEM((n_tok, d), BF16)],
        compiler_params=params(),
        cost_estimate=cost(12 * n_tok * d * f, 12 * d * f + 4 * n_tok * f),
        name='wgrad',
    )(gain, ho, hp, dyo, dyp, w1, w2, u, da)


FIRST_TILES = (21, 18, 12, 9)


def solution(mesh):
    n_stage = mesh.shape['stage']
    n_dp = mesh.shape['dp']
    swap = [(0, 1), (1, 0)]

    def device_step(x_emb, labels, norm_gain, w_up, w_down, w_out):
        n_micro, n_tok, d = x_emb.shape
        own = n_micro * n_tok
        n_voc = w_out.shape[0]
        n_vtile = n_voc // VB
        stage = lax.axis_index('stage')
        dp = lax.axis_index('dp')
        scale = 1.0 / (own * n_dp)
        gain, w1, w2 = norm_gain[0], w_up[0, 0], w_down[0, 0]
        base = (stage * n_voc).reshape(1).astype(jnp.int32)

        def lanes(v):
            return jnp.broadcast_to(v.reshape(own, 1), (own, LANES))

        lab = labels.reshape(own)
        lab_o, lab_p = lanes(lab), lanes(lax.ppermute(lab, 'dp', swap))

        hin, hinp, hfin, gp, u = forward(n_stage, x_emb, gain, w1, w2)
        ho = hfin.reshape(own, d)
        hp = lax.ppermute(ho, 'dp', swap)
        z, stats = logits(base, ho, w_out, lab_o)

        every = lax.all_gather(stats, ('dp', 'stage')).reshape(n_dp, n_stage, 8, own)
        top = jnp.max(every[:, :, 0], axis=1)
        lse = top + jnp.log(jnp.sum(every[:, :, 1] * jnp.exp(every[:, :, 0] - top[:, None]), axis=1))
        loss = jnp.sum(lse - jnp.sum(every[:, :, 2], axis=1)) * scale
        lse_o = lanes(lax.dynamic_index_in_dim(lse, dp, 0, keepdims=False))
        lse_p = lanes(lax.dynamic_index_in_dim(lse, 1 - dp, 0, keepdims=False))

        dzs, tops = [], []
        for half in range(2):
            dz, dh = dhid(scale, half, 2, base, z, w_out, lse_o, lab_o)
            dh = dh + lax.ppermute(dh, 'stage', [(0, 1), (2, 3)])
            dh = dh + lax.ppermute(dh, 'stage', [(1, 3)])
            dzs.append(dz)
            tops.append(dh.astype(BF16).reshape(n_micro // 2, n_tok, d))

        first = jnp.asarray(FIRST_TILES, jnp.int32)[stage].reshape(1)
        s_first = jnp.concatenate([base, jnp.zeros((1,), jnp.int32), first])
        s_rest = jnp.concatenate([base, first, n_vtile - first])
        head = (w_out, dzs[0], dzs[1], ho, hp, lse_p, lab_p)
        gw = dwout(scale, max(FIRST_TILES), s_first, *head)

        tops, gw = lax.optimization_barrier((tops, gw))
        dyin, dyp, da, gx, dg = backward(n_stage, tops, hin, gain, w1, w2, gp)
        gw, dyin = lax.optimization_barrier((gw, dyin))
        gw = dwout(scale, n_vtile - min(FIRST_TILES), s_rest, *head, out=gw)

        gw, gx, dg, dyin = lax.optimization_barrier((gw, gx, dg, dyin))
        dw1, dw2 = wgrad(gain, hin.reshape(own, d), hinp.reshape(own, d), dyin.reshape(own, d), dyp.reshape(own, d), w1, w2, u, da)

        dg = jnp.sum(dg, axis=0)
        dg = dg + lax.ppermute(dg, 'dp', swap)
        grad_x = jnp.where(stage == 0, gx[0], 0.0)
        for k in range(1, n_stage):
            grad_x = grad_x + lax.ppermute(gx[k], 'stage', [(0, k)])
        return loss.reshape(1), grad_x, dg.reshape(1, 1, d), dw1[None, None], dw2[None, None], gw

    tok_spec = ('pod', 'dp')
    stage_spec = ('pod', 'stage')
    rows = P(stage_spec)
    toks = P(None, tok_spec)
    in_specs = (toks, toks, rows, rows, rows, rows)
    out_specs = (P('pod'), P(*toks, 'stage'), rows, rows, rows, rows)
    return jax.shard_map(device_step, mesh=mesh, in_specs=in_specs, out_specs=out_specs, check_vma=False)
```
